256 devices in a mesh: leaf: 64 (over z, y, core), front: 4 (over x).
Axes of the slice: x: 4, y: 4, z: 8, core: 2. Of those that a mesh axis runs over, the one named last changes fastest.
Arguments:
- rhs_leaf: float32 [32, 65536], P(None, ('leaf', 'front')), may hold values from -6 to 6
- rhs_sep: float32 [32, 32768], P(None, ('leaf', 'front')), may hold values from -6 to 6
- inv_leaf: float32 [64, 1024, 1024], P('leaf', 'front'), may hold values from -0.1875 to 0.1875
- inv_sep: float32 [64, 512, 512], P('leaf', 'front'), may hold values from -0.25 to 0.25
- push_leaf: float32 [64, 128, 1024], P('leaf', None, 'front'), may hold values from -0.09375 to 0.09375
- push_sep: float32 [64, 128, 512], P('leaf', None, 'front'), may hold values from -0.125 to 0.125
- pull_leaf: float32 [64, 1024, 128], P('leaf', 'front'), may hold values from -0.25 to 0.25
- pull_sep: float32 [64, 512, 128], P('leaf', 'front'), may hold values from -0.25 to 0.25
- rows_leaf: int32 [64, 128], P('leaf'), may hold values from 0 to 511, as said below
- rows_sep: int32 [64, 128], P('leaf'), may hold values from 0 to 511, as said below
- pivot_leaf: int32 [64, 1024], P('leaf'), may hold values from 0 to 1023, each once within a row
- pivot_sep: int32 [64, 512], P('leaf'), may hold values from 0 to 511, each once within a row
- basis_leaf: float32 [50, 65536], P(None, ('leaf', 'front')), may hold values from -6 to 6
- basis_sep: float32 [50, 32768], P(None, ('leaf', 'front')), may hold values from -6 to 6
Outputs:
- q_leaf: float32 [32, 65536], P(None, ('leaf', 'front'))
- q_sep: float32 [32, 32768], P(None, ('leaf', 'front'))
- coeffs: float32 [50, 32], replicated
- rfac: float32 [32, 32], replicated
The draws below stay inside these ranges and needn't reach their ends.
Inputs may be any that keep to these rules, and one draw needn't show every extreme that they name: `rows_leaf`: each row holds 128 different rows of a separator front. `rows_sep`: each row holds 128 different rows of a separator front. `pivot_leaf`: each row is a permutation. `pivot_sep`: each row is a permutation.
All inputs are finite; a program needn't handle non-finite values.
Results may differ from the reference program's by a relative error of at most 0.0001.
Values sent between devices are 32-bit elements; how exact they have to be, the bound alone decides.
A program may use at most 64 MiB of HBM per device.

```python
import jax
import jax.numpy as jnp
from jax import lax

LEAF_ROWS = 1024
SEP_ROWS = 512
BLOCK = 32
RANK = 50
COUPLE = 128
LEAF_ALL = 65536
SEP_ALL = 32768
N_LEAF = 64


def pick_rows(key):
    scores = jax.random.randint(key, (N_LEAF, SEP_ROWS), 0, 2 ** 18) * SEP_ROWS + jnp.arange(SEP_ROWS, dtype=jnp.int32)[None, :]
    return jnp.argsort(scores, axis=1, stable=True)[:, :COUPLE].astype(jnp.int32)


def draw_rows_leaf(key, part):
    return pick_rows(jax.random.fold_in(key, 101))


def draw_rows_sep(key, part):
    return pick_rows(jax.random.fold_in(key, 202))


def levels(stream_key, shape, pieces, low, largest):
    def one(axis_at, shards_of):
        draws = jax.random.uniform(jax.random.fold_in(jax.random.fold_in(stream_key, 6), axis_at), (shards_of,), jnp.float32, low / len(pieces), largest / len(pieces))
        return jnp.repeat(jnp.exp(draws), shape[axis_at] // shards_of).reshape((-1,) + (1,) * (len(shape) - axis_at - 1))

    level = one(*pieces[0])
    for cut in pieces[1:]:
        level = level * one(*cut)
    return level


def noise(stream_key, dims, width, limit, shards=(), held_as=jnp.bfloat16):
    drawn = width * jax.random.normal(stream_key, dims, jnp.float32)
    if shards:
        drawn = drawn * levels(stream_key, dims, shards, -0.22, 0.18)
    return jnp.clip(drawn, -limit, limit).astype(held_as)


def setup_inputs(seed: int = 0) -> dict:
    streams_of = jax.random.split(jax.random.key(seed), 15)
    return {
        "rhs_leaf": noise(streams_of[0], (BLOCK, LEAF_ALL), 1.0, 6.0, ((1, 256),), jnp.float32),
        "rhs_sep": noise(streams_of[1], (BLOCK, SEP_ALL), 1.0, 6.0, ((1, 256),), jnp.float32),
        "inv_leaf": noise(streams_of[2], (N_LEAF, LEAF_ROWS, LEAF_ROWS), LEAF_ROWS ** -0.5, 0.1875, ((0, 64), (1, 4)), jnp.float32),
        "inv_sep": noise(streams_of[3], (N_LEAF, SEP_ROWS, SEP_ROWS), SEP_ROWS ** -0.5, 0.25, ((0, 64), (1, 4)), jnp.float32),
        "push_leaf": noise(streams_of[4], (N_LEAF, COUPLE, LEAF_ROWS), (4 * LEAF_ROWS) ** -0.5, 0.09375, ((0, 64), (2, 4)), jnp.float32),
        "push_sep": noise(streams_of[5], (N_LEAF, COUPLE, SEP_ROWS), (4 * SEP_ROWS) ** -0.5, 0.125, ((0, 64), (2, 4)), jnp.float32),
        "pull_leaf": noise(streams_of[6], (N_LEAF, LEAF_ROWS, COUPLE), (4 * COUPLE) ** -0.5, 0.25, ((0, 64), (1, 4)), jnp.float32),
        "pull_sep": noise(streams_of[7], (N_LEAF, SEP_ROWS, COUPLE), (4 * COUPLE) ** -0.5, 0.25, ((0, 64), (1, 4)), jnp.float32),
        "rows_leaf": draw_rows_leaf(jax.random.fold_in(streams_of[14], 71), 0),
        "rows_sep": draw_rows_sep(jax.random.fold_in(streams_of[14], 71), 0),
        "pivot_leaf": jax.vmap(lambda own: jax.random.permutation(own, LEAF_ROWS))(jax.random.split(streams_of[10], N_LEAF)).reshape((N_LEAF, LEAF_ROWS)).astype(jnp.int32),
        "pivot_sep": jax.vmap(lambda own: jax.random.permutation(own, SEP_ROWS))(jax.random.split(streams_of[11], N_LEAF)).reshape((N_LEAF, SEP_ROWS)).astype(jnp.int32),
        "basis_leaf": noise(streams_of[12], (RANK, LEAF_ALL), 1.0, 6.0, ((1, 256),), jnp.float32),
        "basis_sep": noise(streams_of[13], (RANK, SEP_ALL), 1.0, 6.0, ((1, 256),), jnp.float32),
    }


exact_mode = lax.Precision.HIGHEST

def contract(former, latter):
    return lax.dot_general(former.astype(jnp.float32), latter.astype(jnp.float32), (((1,), (1,)), ((), ())), precision=exact_mode, preferred_element_type=jnp.float32)

def expand(coeff_block, basis):
    return jnp.dot(coeff_block.T.astype(jnp.float32), basis.astype(jnp.float32), precision=exact_mode, preferred_element_type=jnp.float32)

def apply_inverse(gathered, inverse, pivots):
    return contract(gathered[:, pivots], inverse)

def scatter_rows(partial_term, row_list, sep_width):
    return jnp.zeros((partial_term.shape[0], sep_width), jnp.float32).at[:, row_list].add(partial_term)

def reference(rhs_leaf, rhs_sep, inv_leaf, inv_sep, push_leaf, push_sep, pull_leaf, pull_sep, rows_leaf, rows_sep, pivot_leaf, pivot_sep, basis_leaf, basis_sep):
    groups = N_LEAF
    top_level = groups.bit_length() - 1
    level_of = [top_level + 1] + [(holder & -holder).bit_length() for holder in range(1, groups)]

    def parent_of(holder):
        height = level_of[holder]
        if height == top_level:
            return 0
        return 2 * (holder >> height + 1) + 1 << height
    leaf_rhs = rhs_leaf.reshape(BLOCK, groups, LEAF_ROWS)
    sep_rhs = rhs_sep.reshape(BLOCK, groups, SEP_ROWS)
    leaf_state = [apply_inverse(leaf_rhs[:, holder], inv_leaf[holder], pivot_leaf[holder]) for holder in range(groups)]
    arriving = [jnp.zeros((BLOCK, SEP_ROWS), jnp.float32) for holder in range(groups)]
    for holder in range(groups):
        term = scatter_rows(contract(leaf_state[holder], push_leaf[holder]), rows_leaf[holder], SEP_ROWS)
        arriving[holder | 1] = arriving[holder | 1] + term
    sep_state = [None] * groups
    for height in range(1, top_level + 2):
        for holder in range(groups):
            if level_of[holder] == height:
                sep_state[holder] = apply_inverse(sep_rhs[:, holder] - arriving[holder], inv_sep[holder], pivot_sep[holder])
                if height <= top_level:
                    parent = parent_of(holder)
                    term = scatter_rows(contract(sep_state[holder], push_sep[holder]), rows_sep[holder], SEP_ROWS)
                    arriving[parent] = arriving[parent] + term
    sep_solution = list(sep_state)
    for height in range(top_level, 0, -1):
        for holder in range(groups):
            if level_of[holder] == height:
                above = sep_solution[parent_of(holder)]
                lifted = contract(above[:, rows_sep[holder]], pull_sep[holder])
                sep_solution[holder] = sep_state[holder] - apply_inverse(lifted, inv_sep[holder], pivot_sep[holder])
    leaf_solution = []
    for holder in range(groups):
        lifted = contract(sep_solution[holder | 1][:, rows_leaf[holder]], pull_leaf[holder])
        leaf_solution.append(leaf_state[holder] - apply_inverse(lifted, inv_leaf[holder], pivot_leaf[holder]))
    solved_leaf = jnp.stack(leaf_solution, axis=1).reshape(BLOCK, groups * LEAF_ROWS)
    solved_sep = jnp.stack(sep_solution, axis=1).reshape(BLOCK, groups * SEP_ROWS)
    total_rows = groups * (LEAF_ROWS + SEP_ROWS)
    first_proj = (contract(basis_leaf, solved_leaf) + contract(basis_sep, solved_sep)) / total_rows
    once_leaf = solved_leaf - expand(first_proj, basis_leaf)
    once_sep = solved_sep - expand(first_proj, basis_sep)
    second = (contract(basis_leaf, once_leaf) + contract(basis_sep, once_sep)) / total_rows
    twice_leaf = once_leaf - expand(second, basis_leaf)
    twice_sep = once_sep - expand(second, basis_sep)
    gram_matrix = (contract(twice_leaf, twice_leaf) + contract(twice_sep, twice_sep)) / total_rows
    lower_factor = jnp.linalg.cholesky(gram_matrix)
    q_leaf = lax.linalg.triangular_solve(lower_factor, twice_leaf, left_side=True, lower=True)
    q_sep = lax.linalg.triangular_solve(lower_factor, twice_sep, left_side=True, lower=True)
    return (q_leaf, q_sep, first_proj + second, lower_factor.T)
```

```python
import functools

import jax
import jax.numpy as jnp
from jax import lax
from jax.experimental import pallas as pl
from jax.experimental.pallas import tpu as pltpu
from jax.sharding import Mesh
from jax.sharding import PartitionSpec as P

AXES = ("leaf_0", "leaf_1", "leaf_2", "front")
LEAF = AXES[:3]
F32, BF16 = jnp.float32, jnp.bfloat16
MESH = pl.DeviceIdType.MESH
EXACT = lax.Precision.HIGHEST
BATCH, LEAF_CUT, SEP_CUT, COUPLE = 32, 256, 128, 128
LEAF_ROWS, SEP_ROWS, GROUPS = 1024, 512, 64
TOTAL = GROUPS * (LEAF_ROWS + SEP_ROWS)


def nt(a, b):
    return lax.dot_general(a, b, (((1,), (1,)), ((), ())), precision=EXACT, preferred_element_type=F32)


def nn(a, b):
    return lax.dot_general(a, b, (((1,), (0,)), ((), ())), precision=EXACT, preferred_element_type=F32)


def plain(a, b, last):
    return lax.dot_general(a, b, (((1,), (last,)), ((), ())), preferred_element_type=F32)


def split3(a):
    high = a.astype(BF16)
    rest = a - high.astype(F32)
    mid = rest.astype(BF16)
    low = (rest - mid.astype(F32)).astype(BF16)
    return high, mid, low


def select_from(a, chosen, last):
    rows = a.shape[0]
    pieces = plain(jnp.concatenate(split3(a), axis=0), chosen, last)
    return pieces[:rows] + pieces[rows : 2 * rows] + pieces[2 * rows :]


def select_rows(chosen, a):
    high, mid, low = split3(a)
    return plain(chosen, high, 0) + plain(chosen, mid, 0) + plain(chosen, low, 0)


def ones_where(test):
    return jnp.where(test, 1.0, 0.0).astype(BF16)


def iota(shape, dim):
    return lax.broadcasted_iota(jnp.int32, shape, dim)


def kernel(
    rhs_leaf, rhs_sep, inv_leaf, inv_sep, push_leaf, push_sep, pull_leaf, pull_sep,
    rows_leaf, rows_sep, pivot_leaf, pivot_sep, basis_leaf, basis_sep,
    q_leaf, q_sep, coeffs, rfac,
    v_leaf, v_sep, pulls_sep, pulls_leaf, perm_leaf, sums, m_parts, aep, kid_rows,
    u, y, y_leaf, c_out, yk_out, m_full, gn, ls, z, w2s,
    ar_c, ar_x, ar_y, ar_z, br_c, br_x, br_y, br_z,
    front_send, front_recv, tree_send, tree_recv, ar_send, ar_recv,
):
    zi, yi, ci, fi = (lax.axis_index(name) for name in AXES)
    g = zi * 8 + yi * 2 + ci
    low = jnp.int32(1)
    for k in range(1, 7):
        low = low + (1 - (g % 2**k + 2**k - 1) // 2**k) * 2 ** (k - 1)
    nonroot = (g + 63) // 64
    even = 1 - ci
    parent = ((2 * (g // (4 * low)) + 1) * 2 * low) % GROUPS
    upper = (g // (2 * low)) % 2
    kid_low, kid_high = (g + GROUPS - low // 2) % GROUPS, (g + low // 2) % GROUPS

    def at_group(k):
        return (k // 8, (k // 2) % 4, k % 2, fi)

    partner = (zi, yi, 1 - ci, fi)

    def front_peer(i):
        return (zi, yi, ci, (fi + i) % 4)

    barrier = pltpu.get_barrier_semaphore()

    def greet(device):
        pl.semaphore_signal(barrier, inc=1, device_id=device, device_id_type=MESH)

    for i in range(1, 4):
        greet(front_peer(i))
        greet((zi, (yi + i) % 4, ci, fi))
    for i in range(1, 8):
        greet(((zi + i) % 8, yi, ci, fi))
    greet(partner)

    @pl.when(nonroot == 1)
    def _():
        greet(at_group(parent))

    @pl.when(ci == 0)
    def _():
        greet(at_group(kid_low))

    @pl.when(jnp.logical_and(ci == 0, nonroot == 1))
    def _():
        greet(at_group(kid_high))

    pl.semaphore_wait(barrier, 14 + nonroot + even * (1 + nonroot))

    def remote(src, dst, send, recv, device):
        return pltpu.make_async_remote_copy(
            src_ref=src, dst_ref=dst, send_sem=send, recv_sem=recv, device_id=device, device_id_type=MESH
        )

    def to_front(kind, src, slots):
        return [
            remote(src, slots.at[fi], front_send.at[kind, i - 1], front_recv.at[kind, i - 1], front_peer(i))
            for i in range(1, 4)
        ]

    def start(copies):
        for copy in copies:
            copy.start()

    def from_front(kind, slots):
        for i in range(1, 4):
            slot = slots.at[(fi + 4 - i) % 4]
            remote(slot, slot, front_send.at[kind, i - 1], front_recv.at[kind, i - 1], front_peer(i)).wait_recv()

    def edge(kind, src, dst, device, lands=None):
        return remote(src, dst, tree_send.at[kind], tree_recv.at[kind if lands is None else lands], device)

    sent_leaf = to_front(0, rhs_leaf, v_leaf)
    sent_sep = to_front(1, rhs_sep, v_sep)
    start(sent_leaf)
    start(sent_sep)

    def rows_edge(leaf_side, low_side):
        if leaf_side:
            return edge(0, rows_leaf, kid_rows.at[0], partner)
        if low_side:
            return edge(2, rows_sep, kid_rows.at[0], at_group(parent))
        return edge(3, rows_sep, kid_rows.at[1], at_group(parent))

    is_low = jnp.logical_and(nonroot == 1, upper == 0)
    is_high = jnp.logical_and(nonroot == 1, upper == 1)

    @pl.when(ci == 0)
    def _():
        rows_edge(True, True).start()

    @pl.when(is_low)
    def _():
        rows_edge(False, True).start()

    @pl.when(is_high)
    def _():
        rows_edge(False, False).start()

    sent_pull_sep = to_front(2, pull_sep.at[0], pulls_sep)
    sent_pull_leaf = to_front(3, pull_leaf.at[0], pulls_leaf)
    start(sent_pull_sep)
    start(sent_pull_leaf)

    v_leaf[fi] = rhs_leaf[...]
    v_sep[fi] = rhs_sep[...]
    pulls_sep[fi] = pull_sep[0]
    pulls_leaf[fi] = pull_leaf[0]

    pivots = pivot_leaf[...]
    for s in range(4):
        perm_leaf[s * 256 : (s + 1) * 256] = ones_where(iota((256, LEAF_ROWS), 0) + s * 256 == pivots)
    perm_sep = ones_where(iota((SEP_ROWS, SEP_ROWS), 0) == pivot_sep[...])
    from_front(0, v_leaf)
    moved = select_from(v_leaf[0], perm_leaf[0:256], 0)
    for s in range(1, 4):
        moved = moved + select_from(v_leaf[s], perm_leaf[s * 256 : (s + 1) * 256], 0)
    ls[...] = nt(moved, inv_leaf[0])
    from_front(1, v_sep)
    moved = select_from(v_sep[0], perm_sep[0:128], 0)
    for s in range(1, 4):
        moved = moved + select_from(v_sep[s], perm_sep[s * 128 : (s + 1) * 128], 0)
    s0 = nt(moved, inv_sep[0])
    sums[fi, 0:32] = nt(ls[...], push_leaf[0])
    sums[fi, 32:64] = nt(s0, push_sep[0])
    sums[fi, 64:96] = s0
    sent_sums = to_front(4, sums.at[fi], sums)
    start(sent_sums)

    @pl.when(ci == 1)
    def _():
        kid_rows[1] = rows_leaf[...]
        edge(0, rows_leaf, kid_rows.at[0], partner).wait_recv()

    @pl.when(ci == 0)
    def _():
        edge(2, rows_sep, kid_rows.at[0], partner).wait_recv()

    @pl.when(jnp.logical_and(ci == 0, nonroot == 1))
    def _():
        edge(3, rows_sep, kid_rows.at[1], partner).wait_recv()

    @pl.when(nonroot == 0)
    def _():
        kid_rows[1] = jnp.full((1, COUPLE), -1, jnp.int32)
        u[1] = jnp.zeros((BATCH, COUPLE), F32)
        y[...] = jnp.zeros((BATCH, COUPLE), F32)

    columns = [
        jnp.transpose(jnp.broadcast_to(kid_rows[k].astype(F32), (COUPLE, COUPLE))) for k in range(2)
    ]
    pivots_f = pivot_sep[...].astype(F32)

    def wide(column):
        return jnp.concatenate([column] * 4, axis=1)

    picked = jnp.concatenate(
        [ones_where(wide(column) == pivots_f) for column in columns], axis=0
    )
    chosen = jnp.concatenate(
        [ones_where(wide(column) == iota((COUPLE, SEP_ROWS), 1).astype(F32)) for column in columns], axis=0
    )
    ae = select_from(inv_sep[0], picked, 1)
    m_parts[fi] = nn(push_sep[0], ae)
    sent_m = to_front(5, m_parts.at[fi], m_parts)
    start(sent_m)

    from_front(2, pulls_sep)
    moved = select_from(jnp.transpose(pulls_sep[0]), perm_sep[0:128], 0)
    for s in range(1, 4):
        moved = moved + select_from(jnp.transpose(pulls_sep[s]), perm_sep[s * 128 : (s + 1) * 128], 0)
    ap = nt(inv_sep[0], moved)
    aep[fi, :, 0:256] = ae
    aep[fi, :, 256:384] = ap
    sent_aep = to_front(6, aep.at[fi], aep)
    start(sent_aep)

    from_front(4, sums)
    total = ((sums[0] + sums[1]) + sums[2]) + sums[3]
    d = total[32:64]
    c_out[0] = total[0:32]

    @pl.when(ci == 0)
    def _():
        edge(1, c_out.at[0], u.at[0], partner).start()

    from_front(5, m_parts)
    m_full[...] = ((m_parts[0] + m_parts[1]) + m_parts[2]) + m_parts[3]

    def up():
        both = jnp.concatenate([u[0], u[1]], axis=1)
        c_out[1] = d - nt(both, m_full[...])

        @pl.when(is_low)
        def _():
            edge(4, c_out.at[1], u.at[0], at_group(parent)).start()

        @pl.when(is_high)
        def _():
            edge(5, c_out.at[1], u.at[1], at_group(parent)).start()

    @pl.when(ci == 1)
    def _():
        u[1] = c_out[0]
        edge(1, c_out.at[0], u.at[0], partner).wait_recv()
        up()

    from_front(6, aep)
    found = select_rows(chosen[:, 0:128], aep[0])
    for s in range(1, 4):
        found = found + select_rows(chosen[:, s * 128 : (s + 1) * 128], aep[s])
    gn[...] = found
    s0_all = jnp.concatenate([sums[s, 64:96] for s in range(4)], axis=1)
    r = select_from(s0_all, chosen, 1)
    from_front(3, pulls_leaf)
    moved = select_from(jnp.transpose(pulls_leaf[0]), perm_leaf[0:256], 0)
    for s in range(1, 4):
        moved = moved + select_from(jnp.transpose(pulls_leaf[s]), perm_leaf[s * 256 : (s + 1) * 256], 0)
    ap_leaf = nt(inv_leaf[0], moved)

    z[...] = jnp.zeros_like(z)
    z[64:114, 0:256] = basis_leaf[...]
    z[64:114, 256:384] = basis_sep[...]
    w2s[...] = jnp.zeros_like(w2s)

    @pl.when(ci == 0)
    def _():
        edge(4, c_out.at[1], u.at[0], partner).wait_recv()

    @pl.when(jnp.logical_and(ci == 0, nonroot == 1))
    def _():
        edge(5, c_out.at[1], u.at[1], partner).wait_recv()

    @pl.when(ci == 0)
    def _():
        up()

    both = jnp.concatenate([u[0], u[1]], axis=1)
    waiting = r - nt(both, gn[:, 0:256])

    @pl.when(nonroot == 1)
    def _():
        edge(6, yk_out.at[0], y, partner).wait_recv()

    below = waiting - nt(y[...], gn[:, 256:384])
    yk_out[0] = below[:, 0:128]
    yk_out[1] = below[:, 128:256]

    @pl.when(ci == 1)
    def _():
        edge(7, yk_out.at[0], y_leaf, partner).start()
        y_leaf[...] = yk_out[1]

    @pl.when(ci == 0)
    def _():
        edge(6, yk_out.at[0], y, at_group(kid_low)).start()

    @pl.when(jnp.logical_and(ci == 0, nonroot == 1))
    def _():
        edge(8, yk_out.at[1], y, at_group(kid_high), 6).start()

    x_sep = s0 - nt(jnp.concatenate([both, y[...]], axis=1), aep[fi])

    @pl.when(ci == 0)
    def _():
        edge(7, yk_out.at[0], y_leaf, partner).wait_recv()

    x_leaf = ls[...] - nt(y_leaf[...], ap_leaf)
    z[0:32, 0:256] = x_leaf
    z[0:32, 256:384] = x_sep

    sent_sum = []

    def everywhere(first_sem, value, slots):
        places = ((2, ci, lambda k: (zi, yi, k, fi)), (4, fi, lambda k: (zi, yi, ci, k)),
                  (4, yi, lambda k: (zi, k, ci, fi)), (8, zi, lambda k: (k, yi, ci, fi)))
        sem = first_sem
        for (count, mine, device), slot in zip(places, slots):
            slot[mine] = value
            copies = []
            for i in range(1, count):
                copies.append(
                    remote(slot.at[mine], slot.at[mine], ar_send.at[sem + i], ar_recv.at[sem + i],
                           device((mine + i) % count))
                )
                copies[-1].start()
            for i in range(1, count):
                came = slot.at[(mine + count - i) % count]
                remote(came, came, ar_send.at[sem + i], ar_recv.at[sem + i], device((mine + i) % count)).wait_recv()
            sent_sum.extend(copies)
            sem += count
            value = slot[0]
            for k in range(1, count):
                value = value + slot[k]
        return value * (1.0 / TOTAL)

    lane = iota((BATCH, 128), 1)
    row = iota((BATCH, 128), 0)
    w = z[0:32]
    rows_in = jnp.concatenate([w, z[64:128]], axis=0)
    found = everywhere(0, nt(rows_in, z[...]), (ar_c, ar_x, ar_y, ar_z))
    first = jnp.where(lane >= 64, found[0:32], 0.0)
    metric = jnp.concatenate(
        [jnp.zeros((64, 128), F32), jnp.where(iota((64, 128), 1) >= 64, found[32:96], 0.0)], axis=0
    )
    once = w - nn(first, z[...])
    z[0:32] = once
    found = everywhere(18, nt(once, z[...]), (br_c, br_x, br_y, br_z))
    second = jnp.where(lane >= 64, found, 0.0)
    own = jnp.where(lane < 32, found, 0.0)
    second_rows = jnp.concatenate([second, jnp.zeros((96, 128), F32)], axis=0)
    gram = own + nt(nn(second, metric) - 2.0 * second, second_rows)
    w2s[32:64] = once - nn(second, z[...])

    work = gram + jnp.where(lane == row + 32, 1.0, 0.0)
    for j in range(BATCH):
        pivot = work[j : j + 1, j : j + 1]
        root = lax.rsqrt(pivot)
        root = root * (1.5 - 0.5 * pivot * root * root)
        line = work[j : j + 1, :] * root
        column = work[:, j : j + 1] * root
        work = jnp.where(row > j, work - column * line, jnp.where(row == j, line, work))
    q = nn(jnp.where(jnp.logical_and(lane >= 32, lane < 64), work, 0.0), w2s[...])
    q_leaf[...] = q[:, 0:256]
    q_sep[...] = q[:, 256:384]
    rfac[...] = jnp.where(lane >= row, work, 0.0)[:, 0:32]
    coeff = jnp.transpose(jnp.concatenate([first + second, jnp.zeros((96, 128), F32)], axis=0))
    coeffs[...] = coeff[64:114, 0:32]

    for copies in (sent_leaf, sent_sep, sent_pull_sep, sent_pull_leaf, sent_sums, sent_m, sent_aep, sent_sum):
        for copy in copies:
            copy.wait_send()

    @pl.when(ci == 0)
    def _():
        rows_edge(True, True).wait_send()
        edge(1, c_out.at[0], u.at[0], partner).wait_send()
        edge(6, yk_out.at[0], y, partner).wait_send()

    @pl.when(jnp.logical_and(ci == 0, nonroot == 1))
    def _():
        edge(8, yk_out.at[1], y, partner).wait_send()

    @pl.when(ci == 1)
    def _():
        edge(7, yk_out.at[0], y_leaf, partner).wait_send()

    @pl.when(is_low)
    def _():
        rows_edge(False, True).wait_send()
        edge(4, c_out.at[1], u.at[0], partner).wait_send()

    @pl.when(is_high)
    def _():
        rows_edge(False, False).wait_send()
        edge(5, c_out.at[1], u.at[1], partner).wait_send()


def on_device(*arrays):
    vmem = pl.BlockSpec(memory_space=pltpu.VMEM)
    block = pltpu.VMEM((BATCH, COUPLE), F32)

    def shaped(*dims):
        return pltpu.VMEM(dims, F32)

    return pl.pallas_call(
        kernel,
        out_shape=(
            jax.ShapeDtypeStruct((BATCH, LEAF_CUT), F32),
            jax.ShapeDtypeStruct((BATCH, SEP_CUT), F32),
            jax.ShapeDtypeStruct((50, BATCH), F32),
            jax.ShapeDtypeStruct((BATCH, BATCH), F32),
        ),
        in_specs=[vmem] * 14,
        out_specs=(vmem,) * 4,
        scratch_shapes=[
            shaped(4, 32, 256), shaped(4, 32, 128), shaped(4, 128, 128), shaped(4, 256, 128),
            pltpu.VMEM((1024, 1024), BF16), shaped(4, 96, 128), shaped(4, 128, 256), shaped(4, 128, 384),
            pltpu.VMEM((2, 1, 128), jnp.int32),
            shaped(2, 32, 128), block, block, shaped(2, 32, 128), shaped(2, 32, 128),
            shaped(128, 256), shaped(256, 384), shaped(32, 256), shaped(128, 384), shaped(128, 384),
            shaped(2, 96, 128), shaped(4, 96, 128), shaped(4, 96, 128), shaped(8, 96, 128),
            shaped(2, 32, 128), shaped(4, 32, 128), shaped(4, 32, 128), shaped(8, 32, 128),
            pltpu.SemaphoreType.DMA((7, 3)), pltpu.SemaphoreType.DMA((7, 3)),
            pltpu.SemaphoreType.DMA((9,)), pltpu.SemaphoreType.DMA((9,)),
            pltpu.SemaphoreType.DMA((36,)), pltpu.SemaphoreType.DMA((36,)),
        ],
        compiler_params=pltpu.CompilerParams(collective_id=0, has_side_effects=True),
    )(*arrays)


def solution(mesh):
    torus = Mesh(mesh.devices.reshape(8, 4, 2, 4), AXES)
    return jax.shard_map(
        on_device,
        mesh=torus,
        in_specs=(
            P(None, AXES), P(None, AXES),
            P(LEAF, "front", None), P(LEAF, "front", None),
            P(LEAF, None, "front"), P(LEAF, None, "front"),
            P(LEAF, "front", None), P(LEAF, "front", None),
            P(LEAF, None), P(LEAF, None), P(LEAF, None), P(LEAF, None),
            P(None, AXES), P(None, AXES),
        ),
        out_specs=(P(None, AXES), P(None, AXES), P(), P()),
        check_vma=False,
    )
```
